32 devices in a mesh: batch: 4 (over z), row: 4 (over x, core), col: 2 (over y).
Axes of the slice: x: 2, y: 2, z: 4, core: 2. Of those that a mesh axis runs over, the one named last changes fastest.
Arguments:
- flows: float32 [32768, 8192], P(('batch', 'row'), 'col'), parts along dimension 0, may hold values from 0 to 21, as said below
- tile_mask: int32 [256, 64], P(('batch', 'row'), 'col'), parts along dimension 0, may hold values from 0 to 1, as said below
- row_target: int32 [32768], P(('batch', 'row')), parts along dimension 0, may hold values from 1638400 to 8191999
- col_target: int32 [32768], P(('batch', 'col')), parts along dimension 0, may hold values from 1638400 to 8191999
Outputs:
- row_history: float32 [12, 8192], P('batch', 'row'), parts along dimension 0
- col_history: float32 [12, 8192], P('batch', 'col'), parts along dimension 0
The draws below stay inside these ranges and needn't reach their ends.
There are 4 independent parts, one for each index of `batch`. The reference program is written for one: setup_inputs(seed, part) draws one part's arguments, and reference() takes and returns one part's arrays. A program takes and returns all parts, laid end to end along the dimension named above; each array names one. Nothing has to cross between parts.
Inputs may be any that keep to these rules, and one draw needn't show every extreme that they name: `tile_mask`: every diagonal tile is 1. `flows`: every entry is positive.
All inputs are finite; a program needn't handle non-finite values.
Results may differ from the reference program's by a relative error of at most 0.0001.
Values sent between devices are 32-bit elements; how exact they have to be, the bound alone decides.
A program may use at most 192 MiB of HBM per device.

```python
import jax
import jax.numpy as jnp

N = 8192
TILE = 128
ITERS = 3
TILES = 64


def draw_tile_mask(key, part):
    bits = jax.random.randint(jax.random.fold_in(key, 7), (TILES, TILES), 0, 2, dtype=jnp.int32)
    return jnp.maximum(bits, jnp.eye(TILES, dtype=jnp.int32))


def draw_flows(key, part):
    base_key = jax.random.fold_in(key, 23)
    row_key, col_key, noise_key, sign_key = jax.random.split(base_key, 4)
    row_place = jax.random.uniform(row_key, (TILES,), jnp.float32, -1.0, 1.0)
    col_place = jax.random.uniform(col_key, (TILES,), jnp.float32, -1.0, 1.0)
    roughness = jnp.exp(jax.random.uniform(noise_key, (N, N), jnp.float32, -9.2, 0.0))
    levels = jnp.exp(3.0 * row_place[:, None] * col_place[None, :])
    shaped = roughness.reshape(TILES, TILE, TILES, TILE) * levels[:, None, :, None]
    return shaped.reshape(N, N).astype(jnp.float32)


def set_ends(values, rng, smallest, top_value):
    extent = values.shape
    index_at = [jax.random.randint(jax.random.fold_in(rng, axis), (), 0, extent[axis]) for axis in range(len(extent))]
    values = values.at[tuple(index_at)].set(smallest)
    longest = extent.index(max(extent))
    index_at[longest] = (index_at[longest] + 1) % extent[longest]
    return values.at[tuple(index_at)].set(top_value)


def setup_inputs(seed: int = 0, part: int = 0) -> dict:
    key_list = jax.random.split(jax.random.key(seed), 5)
    part_splits = jax.random.split(jax.random.fold_in(key_list[4], part), 5)
    flows = draw_flows(jax.random.fold_in(jax.random.fold_in(key_list[4], part), 71), part)
    tile_mask = draw_tile_mask(jax.random.fold_in(jax.random.fold_in(key_list[4], part), 71), part)
    row_target = set_ends(jax.random.randint(part_splits[2], (N,), 200 * N, 1000 * N), jax.random.fold_in(part_splits[2], 1), 200 * N, (1000 * N) - 1).astype(jnp.int32)
    col_target = set_ends(jax.random.randint(part_splits[3], (N,), 200 * N, 1000 * N), jax.random.fold_in(part_splits[3], 1), 200 * N, (1000 * N) - 1).astype(jnp.int32)
    return dict(flows=flows, tile_mask=tile_mask, row_target=row_target, col_target=col_target)


def reference(flows, tile_mask, row_target, col_target):
    tiles = tile_mask.shape[0]
    tile = flows.shape[0] // tiles
    expand = tile_mask.astype(jnp.float32)[:, None, :, None]
    active = (flows.reshape(tiles, tile, tiles, tile) * expand).reshape(flows.shape)
    row_goal = row_target.astype(jnp.float32) * 0.001
    col_goal = col_target.astype(jnp.float32) * 0.001
    col_scale = jnp.ones((flows.shape[1],), jnp.float32)
    row_list = []
    col_list = []
    for sweep_index in range(ITERS):
        row_total = jnp.sum(active * col_scale[None, :], axis=1)
        row_scale = row_goal / row_total
        col_total = jnp.sum(active * row_scale[:, None], axis=0)
        col_scale = col_goal / col_total
        row_list.append(row_scale)
        col_list.append(col_scale)
    return jnp.stack(row_list), jnp.stack(col_list)
```

```python
import functools

import jax
import jax.numpy as jnp
from jax import lax
from jax.experimental import pallas as pl
from jax.experimental.pallas import tpu as pltpu
from jax.sharding import PartitionSpec as P

ITERS = 3
LANES = 128
MESH = pl.DeviceIdType.MESH


def pairwise(terms):
    while len(terms) > 1:
        terms = [
            terms[i] + terms[i + 1] if i + 1 < len(terms) else terms[i]
            for i in range(0, len(terms), 2)
        ]
    return terms[0]


def kernel(
    row_n, col_n, flows, mask, row_target, col_target, row_out, col_out,
    held, row_slots, col_slots, row_scale, col_scale, col_acc,
    load_sem, row_send, row_recv, col_send, col_recv,
):
    row_count, col_count = flows.shape
    row_tiles, col_tiles = row_count // LANES, col_count // LANES
    my_row, my_col = lax.axis_index("row"), lax.axis_index("col")

    loads = []
    for b in range(row_tiles):
        rows = pl.ds(b * LANES, LANES)
        load = pltpu.make_async_copy(flows.at[rows, :], held.at[rows, :], load_sem.at[b])
        load.start()
        loads.append(load)

    barrier = pltpu.get_barrier_semaphore()
    for d in range(1, col_n):
        pl.semaphore_signal(
            barrier, inc=1, device_id={"col": lax.rem(my_col + d, col_n)}, device_id_type=MESH
        )
    for d in range(1, row_n):
        pl.semaphore_signal(
            barrier, inc=1, device_id={"row": lax.rem(my_row + d, row_n)}, device_id_type=MESH
        )

    def block(b):
        return pl.ds(pl.multiple_of(b * LANES, LANES), LANES)

    def put_row_total(it, b, acc):
        row_slots[it, my_col, pl.ds(b, 1), :] = jnp.sum(acc.T, axis=0, keepdims=True)

    def exchange(slots, send, recv, it, axis, me, n):
        copies = []
        for d in range(1, n):
            copy = pltpu.make_async_remote_copy(
                src_ref=slots.at[it, me],
                dst_ref=slots.at[it, me],
                send_sem=send.at[it, d],
                recv_sem=recv.at[it, d],
                device_id={axis: lax.rem(me + d, n)},
                device_id_type=MESH,
            )
            copy.start()
            copies.append(copy)
        return copies

    for b in range(row_tiles):
        loads[b].wait()
        acc = jnp.zeros((LANES, LANES), jnp.float32)
        rows = slice(b * LANES, (b + 1) * LANES)
        for j in range(col_tiles):
            cols = slice(j * LANES, (j + 1) * LANES)
            value = held[rows, cols] * mask[b, j].astype(jnp.float32)
            held[rows, cols] = value
            acc = acc + value
        put_row_total(0, b, acc)

    pl.semaphore_wait(barrier, row_n + col_n - 2)

    unroll = 4 if row_tiles % 4 == 0 else 1
    sent = []
    for it in range(ITERS):
        if it > 0:
            def row_pass(step, carry):
                for u in range(unroll):
                    b = step * unroll + u
                    acc = None
                    for j in range(col_tiles):
                        cols = slice(j * LANES, (j + 1) * LANES)
                        term = held[block(b), cols] * col_scale[j : j + 1, :]
                        acc = term if acc is None else acc + term
                    put_row_total(it, b, acc)
                return carry

            lax.fori_loop(0, row_tiles // unroll, row_pass, 0)
        copies = exchange(row_slots, row_send, row_recv, it, "col", my_col, col_n)
        for copy in copies:
            copy.wait_recv()
        sent += copies
        total = pairwise([row_slots[it, k] for k in range(col_n)])
        row_scale[...] = (row_target[...].astype(jnp.float32) * 0.001) / total

        col_acc[...] = jnp.zeros_like(col_acc)

        def col_pass(step, carry):
            for u in range(unroll):
                b = step * unroll + u
                scale = jnp.broadcast_to(row_scale[pl.ds(b, 1), :], (LANES, LANES)).T
                for j in range(col_tiles):
                    cols = slice(j * LANES, (j + 1) * LANES)
                    term = held[block(b), cols] * scale
                    col_acc[j] += pairwise([term[g * 8 : g * 8 + 8] for g in range(LANES // 8)])
            return carry

        lax.fori_loop(0, row_tiles // unroll, col_pass, 0)
        col_slots[it, my_row] = jnp.sum(col_acc[...], axis=1)
        copies = exchange(col_slots, col_send, col_recv, it, "row", my_row, row_n)
        for b in range(row_tiles):
            row_out[it : it + 1, b * LANES : (b + 1) * LANES] = row_scale[b : b + 1, :]
        for copy in copies:
            copy.wait_recv()
        sent += copies
        total = pairwise([col_slots[it, k] for k in range(row_n)])
        col_scale[...] = (col_target[...].astype(jnp.float32) * 0.001) / total
        for j in range(col_tiles):
            col_out[it : it + 1, j * LANES : (j + 1) * LANES] = col_scale[j : j + 1, :]

    for copy in sent:
        copy.wait_send()


def shards(row_n, col_n, flows, tile_mask, row_target, col_target):
    row_count, col_count = flows.shape
    row_tiles, col_tiles = row_count // LANES, col_count // LANES
    vmem = pl.BlockSpec(memory_space=pltpu.VMEM)
    return pl.pallas_call(
        functools.partial(kernel, row_n, col_n),
        out_shape=(
            jax.ShapeDtypeStruct((ITERS, row_count), jnp.float32),
            jax.ShapeDtypeStruct((ITERS, col_count), jnp.float32),
        ),
        in_specs=[
            pl.BlockSpec(memory_space=pl.ANY),
            pl.BlockSpec(memory_space=pltpu.SMEM),
            vmem,
            vmem,
        ],
        out_specs=(vmem, vmem),
        scratch_shapes=[
            pltpu.VMEM((row_count, col_count), jnp.float32),
            pltpu.VMEM((ITERS, col_n, row_tiles, LANES), jnp.float32),
            pltpu.VMEM((ITERS, row_n, col_tiles, LANES), jnp.float32),
            pltpu.VMEM((row_tiles, LANES), jnp.float32),
            pltpu.VMEM((col_tiles, LANES), jnp.float32),
            pltpu.VMEM((col_tiles, 8, LANES), jnp.float32),
            pltpu.SemaphoreType.DMA((row_tiles,)),
            pltpu.SemaphoreType.DMA((ITERS, col_n)),
            pltpu.SemaphoreType.DMA((ITERS, col_n)),
            pltpu.SemaphoreType.DMA((ITERS, row_n)),
            pltpu.SemaphoreType.DMA((ITERS, row_n)),
        ],
        compiler_params=pltpu.CompilerParams(
            collective_id=0, has_side_effects=True, vmem_limit_bytes=60 * 1024 * 1024
        ),
    )(
        flows,
        tile_mask,
        row_target.reshape(row_tiles, LANES),
        col_target.reshape(col_tiles, LANES),
    )


def solution(mesh):
    return jax.shard_map(
        functools.partial(shards, mesh.shape["row"], mesh.shape["col"]),
        mesh=mesh,
        in_specs=(
            P(("batch", "row"), "col"),
            P(("batch", "row"), "col"),
            P(("batch", "row")),
            P(("batch", "col")),
        ),
        out_specs=(P("batch", "row"), P("batch", "col")),
        check_vma=False,
    )
```

```python
import functools

import jax
import jax.numpy as jnp
from jax import lax
from jax.experimental import pallas as pl
from jax.experimental.pallas import tpu as pltpu
from jax.sharding import PartitionSpec as P

ITERS = 3
LANES = 128
LAG = 3
MESH = pl.DeviceIdType.MESH


def pairwise(terms):
    while len(terms) > 1:
        terms = [
            terms[i] + terms[i + 1] if i + 1 < len(terms) else terms[i]
            for i in range(0, len(terms), 2)
        ]
    return terms[0]


def pieces_of(tiles, first):
    return [(0, first), (first, tiles)] if 0 < first < tiles else [(0, tiles)]


def kernel(
    row_n, col_n, flows, mask_in, row_target_in, col_target_in, row_hist, col_hist,
    held, first_slots, row_slots, col_slots, row_acc, col_acc, row_target, col_target, mask,
    load_sem, small_sem, first_send, first_recv, row_send, row_recv, col_send, col_recv,
):
    row_count, col_count = flows.shape
    row_tiles, col_tiles = row_count // LANES, col_count // LANES
    my_row, my_col = lax.axis_index("row"), lax.axis_index("col")
    chunks = first_slots.shape[1]
    per = row_tiles // chunks
    row_pieces = pieces_of(row_tiles, row_tiles // 16 * 8)
    col_pieces = pieces_of(col_tiles, col_tiles // 32 * 8)

    smalls = [
        pltpu.make_async_copy(source, target, small_sem.at[i])
        for i, (source, target) in enumerate(
            [(mask_in, mask), (row_target_in, row_target), (col_target_in, col_target)]
        )
    ]
    smalls[0].start()

    def load(k):
        rows = pl.ds(pl.multiple_of(k * per * LANES, LANES), per * LANES)
        return pltpu.make_async_copy(flows.at[rows, :], held.at[rows, :], load_sem.at[k])

    for k in range(chunks):
        load(k).start()
        if k == 0:
            smalls[1].start()
            smalls[2].start()

    barrier = pltpu.get_barrier_semaphore()
    for d in range(1, col_n):
        pl.semaphore_signal(
            barrier, inc=1, device_id={"col": lax.rem(my_col + d, col_n)}, device_id_type=MESH
        )
    for d in range(1, row_n):
        pl.semaphore_signal(
            barrier, inc=1, device_id={"row": lax.rem(my_row + d, row_n)}, device_id_type=MESH
        )
    first_slots[my_col] = jnp.zeros(first_slots.shape[1:], jnp.float32)
    col_acc[...] = jnp.zeros_like(col_acc)
    for small in smalls:
        small.wait()
    pl.semaphore_wait(barrier, row_n + col_n - 2)

    def block(b):
        return pl.ds(pl.multiple_of(b * LANES, LANES), LANES)

    def lanes(j):
        return slice(j * LANES, (j + 1) * LANES)

    def remote(ref, send, recv, axis, me, n, d):
        return pltpu.make_async_remote_copy(
            src_ref=ref,
            dst_ref=ref,
            send_sem=send.at[d],
            recv_sem=recv.at[d],
            device_id={axis: lax.rem(me + d, n)},
            device_id_type=MESH,
        )

    def first_copies(k):
        return [
            remote(
                first_slots.at[my_col, k], first_send.at[k], first_recv.at[k],
                "col", my_col, col_n, d,
            )
            for d in range(1, col_n)
        ]

    def row_copies(it, p):
        lo, hi = row_pieces[p]
        return [
            remote(
                row_slots.at[it, my_col, pl.ds(lo, hi - lo)], row_send.at[it, p],
                row_recv.at[it, p], "col", my_col, col_n, d,
            )
            for d in range(1, col_n)
        ]

    def col_copies(it, p):
        lo, hi = col_pieces[p]
        return [
            remote(
                col_slots.at[it, my_row, pl.ds(lo, hi - lo)], col_send.at[it, p],
                col_recv.at[it, p], "row", my_row, row_n, d,
            )
            for d in range(1, row_n)
        ]

    def start(copies):
        for copy in copies:
            copy.start()

    def arrive(copies):
        for copy in copies:
            copy.wait_recv()

    def add_cols(it, b, lo, hi):
        scale = jnp.broadcast_to(row_hist[it, pl.ds(b, 1), :], (LANES, LANES)).T
        for j in range(lo, hi):
            term = held[block(b), lanes(j)] * scale
            col_acc[j] += pairwise([term[g * 8 : g * 8 + 8] for g in range(LANES // 8)])

    def loop(lo, hi, body):
        count = hi - lo
        unroll = 4 if count % 4 == 0 else (2 if count % 2 == 0 else 1)

        def steps(step, carry):
            for u in range(unroll):
                body(lo + step * unroll + u)
            return carry

        lax.fori_loop(0, count // unroll, steps, 0)

    def send_cols(it, p):
        lo, hi = col_pieces[p]
        col_slots[it, my_row, lo:hi] = jnp.sum(col_acc[lo:hi], axis=1)
        start(col_copies(it, p))
        col_acc[lo:hi] = jnp.zeros((hi - lo, 8, LANES), jnp.float32)

    def take_cols(it, p):
        arrive(col_copies(it, p))
        lo, hi = col_pieces[p]
        total = pairwise([col_slots[it, m, lo:hi] for m in range(row_n)])
        col_hist[it, lo:hi] = (col_target[lo:hi].astype(jnp.float32) * 0.001) / total

    def first_rows(k):
        load(k).wait()
        for u in range(per):
            b = k * per + u
            acc = None
            for j in range(col_tiles):
                value = held[block(b), lanes(j)] * mask[b, j].astype(jnp.float32)
                held[block(b), lanes(j)] = value
                acc = value if acc is None else acc + value
            first_slots[my_col, k, u : u + 1, :] = jnp.sum(acc.T, axis=0, keepdims=True)
        start(first_copies(k))

    def first_take(k):
        arrive(first_copies(k))
        for u in range(per):
            b = k * per + u
            total = pairwise([first_slots[m, k, u : u + 1, :] for m in range(col_n)])
            goal = row_target[pl.ds(b, 1), :].astype(jnp.float32) * 0.001
            row_hist[0, pl.ds(b, 1), :] = goal / total

    def first_cols(k):
        first_take(k)
        for u in range(per):
            add_cols(0, k * per + u, 0, col_tiles)

    def prologue(k, carry):
        first_rows(k)
        return carry

    def steady(k, carry):
        first_rows(k)
        first_cols(k - LAG)
        return carry

    def epilogue(k, carry):
        first_cols(k)
        return carry

    lax.fori_loop(0, LAG, prologue, 0)
    lax.fori_loop(LAG, chunks, steady, 0)
    lax.fori_loop(chunks - LAG, chunks - 1, epilogue, 0)
    first_take(chunks - 1)
    for p, (lo, hi) in enumerate(col_pieces):
        for u in range(per):
            add_cols(0, (chunks - 1) * per + u, lo, hi)
        send_cols(0, p)

    def row_block(it, b, lo, hi, fresh):
        acc = None if fresh else row_acc[block(b), :]
        for j in range(lo, hi):
            term = held[block(b), lanes(j)] * col_hist[it - 1, j : j + 1, :]
            acc = term if acc is None else acc + term
        return acc

    for it in range(1, ITERS):
        for p, (lo, hi) in enumerate(col_pieces[:-1]):
            take_cols(it - 1, p)

            def partial(b):
                row_acc[block(b), :] = row_block(it, b, lo, hi, p == 0)

            loop(0, row_tiles, partial)
        last = len(col_pieces) - 1
        take_cols(it - 1, last)
        lo, hi = col_pieces[last]
        for p, (top, end) in enumerate(row_pieces):

            def whole(b):
                acc = row_block(it, b, lo, hi, last == 0)
                row_slots[it, my_col, pl.ds(b, 1), :] = jnp.sum(acc.T, axis=0, keepdims=True)

            loop(top, end, whole)
            start(row_copies(it, p))
        for p, (top, end) in enumerate(row_pieces):
            arrive(row_copies(it, p))
            total = pairwise([row_slots[it, m, top:end] for m in range(col_n)])
            row_hist[it, top:end] = (row_target[top:end].astype(jnp.float32) * 0.001) / total
            if p < len(row_pieces) - 1:
                loop(top, end, lambda b: add_cols(it, b, 0, col_tiles))
            else:
                for q, (lo, hi) in enumerate(col_pieces):
                    loop(top, end, lambda b: add_cols(it, b, lo, hi))
                    send_cols(it, q)

    for p in range(len(col_pieces)):
        take_cols(ITERS - 1, p)

    def drain(k, carry):
        for copy in first_copies(k):
            copy.wait_send()
        return carry

    lax.fori_loop(0, chunks, drain, 0)
    for it in range(ITERS):
        copies = [copy for p in range(len(col_pieces)) for copy in col_copies(it, p)]
        if it > 0:
            copies += [copy for p in range(len(row_pieces)) for copy in row_copies(it, p)]
        for copy in copies:
            copy.wait_send()


def close(row_hist, col_hist, row_out, col_out):
    for source, target in ((row_hist, row_out), (col_hist, col_out)):
        for j in range(source.shape[1]):
            target[:, j * LANES : (j + 1) * LANES] = source[:, j, :]


def shards(row_n, col_n, flows, tile_mask, row_target, col_target):
    row_count, col_count = flows.shape
    row_tiles, col_tiles = row_count // LANES, col_count // LANES
    chunks = row_tiles // 2 if row_tiles % 2 == 0 else row_tiles
    vmem = pl.BlockSpec(memory_space=pltpu.VMEM)
    dma = pltpu.SemaphoreType.DMA
    row_hist, col_hist = pl.pallas_call(
        functools.partial(kernel, row_n, col_n),
        out_shape=(
            pltpu.VMEM((ITERS, row_tiles, LANES), jnp.float32),
            pltpu.VMEM((ITERS, col_tiles, LANES), jnp.float32),
        ),
        in_specs=[pl.BlockSpec(memory_space=pl.ANY)] * 4,
        out_specs=(vmem, vmem),
        scratch_shapes=[
            pltpu.VMEM((row_count, col_count), jnp.float32),
            pltpu.VMEM((col_n, chunks, 8, LANES), jnp.float32),
            pltpu.VMEM((ITERS, col_n, row_tiles, LANES), jnp.float32),
            pltpu.VMEM((ITERS, row_n, col_tiles, LANES), jnp.float32),
            pltpu.VMEM((row_count, LANES), jnp.float32),
            pltpu.VMEM((col_tiles, 8, LANES), jnp.float32),
            pltpu.VMEM((row_tiles, LANES), jnp.int32),
            pltpu.VMEM((col_tiles, LANES), jnp.int32),
            pltpu.SMEM((row_tiles, col_tiles), jnp.int32),
            dma((chunks,)),
            dma((3,)),
            dma((chunks, col_n)),
            dma((chunks, col_n)),
            dma((ITERS, 2, col_n)),
            dma((ITERS, 2, col_n)),
            dma((ITERS, 2, row_n)),
            dma((ITERS, 2, row_n)),
        ],
        compiler_params=pltpu.CompilerParams(
            collective_id=0, has_side_effects=True, vmem_limit_bytes=56 * 1024 * 1024
        ),
    )(
        flows,
        tile_mask,
        row_target.reshape(row_tiles, LANES),
        col_target.reshape(col_tiles, LANES),
    )
    return pl.pallas_call(
        close,
        out_shape=(
            jax.ShapeDtypeStruct((ITERS, row_count), jnp.float32),
            jax.ShapeDtypeStruct((ITERS, col_count), jnp.float32),
        ),
        in_specs=[vmem, vmem],
        out_specs=(vmem, vmem),
    )(*(pltpu.with_memory_space_constraint(h, pltpu.VMEM) for h in (row_hist, col_hist)))


def solution(mesh):
    return jax.shard_map(
        functools.partial(shards, mesh.shape["row"], mesh.shape["col"]),
        mesh=mesh,
        in_specs=(
            P(("batch", "row"), "col"),
            P(("batch", "row"), "col"),
            P(("batch", "row")),
            P(("batch", "col")),
        ),
        out_specs=(P("batch", "row"), P("batch", "col")),
        check_vma=False,
    )
```
